32 devices in a mesh: groups: 2 (over y), seq: 4 (over z), head: 4 (over x, core).
Axes of the slice: x: 2, y: 2, z: 4, core: 2. Of those that a mesh axis runs over, the one named last changes fastest.
Arguments:
- queries: bfloat16 [1536, 16, 576], P(('groups', 'seq'), 'head'), parts along dimension 0, may hold values from -40 to 40
- latent_kv: bfloat16 [1536, 576], P(('groups', 'seq')), parts along dimension 0, may hold values from -6 to 6
- adapter_ids: int32 [48], P(('groups', 'seq')), parts along dimension 0, may hold values from 0 to 4
- value_up: bfloat16 [16, 512, 128], P('head'), may hold values from -0.25 to 0.25
- output_weight: bfloat16 [2048, 2048], P('head'), may hold values from -0.1875 to 0.1875
- adapter_down: bfloat16 [2048, 80], P('head'), may hold values from -0.125 to 0.125
- adapter_up: bfloat16 [80, 2048], replicated, may hold values from -1.5 to 1.5
Outputs:
- mixed: bfloat16 [1536, 2048], P(('groups', 'seq'), 'head'), parts along dimension 0
The draws below stay inside these ranges and needn't reach their ends.
There are 2 independent parts, one for each index of `groups`. The reference program is written for one: setup_inputs(seed, part) draws one part's arguments, and reference() takes and returns one part's arrays. A program takes and returns all parts, laid end to end along the dimension named above; an argument that names none is the same for every part. Nothing has to cross between parts.
All inputs are finite; a program needn't handle non-finite values.
Results may differ from the reference program's by a relative error of at most 0.017.
Values may be sent and summed in bfloat16 or wider, within the bound.
No kernel may reach another device: no remote copies, remote signals or barrier semaphores. Data moves between devices by JAX's collectives and lax.ppermute only.
A program may use at most 64 MiB of HBM per device.

```python
import math
import jax
import jax.numpy as jnp
from jax import lax

D = 2048
HEADS = 16
LATENT = 512
ROPE = 64
NOPE = 128
VHEAD = 128
ADAPTERS = 5
RANK = 16
ADP_BLOCK = 32
TOK_DEV = 192
TOKENS = 768
N_SEQ = 4


def pair_draws(key):
    base = jax.random.fold_in(key, 11)
    first_key, second_key = jax.random.split(base, 2)
    latent_width = LATENT + ROPE
    latent = jnp.clip(jax.random.normal(first_key, (TOKENS, latent_width), jnp.float32), -6.0, 6.0)
    queries = jnp.clip(jax.random.normal(second_key, (TOKENS, HEADS, latent_width), jnp.float32), -6.0, 6.0)
    queries = jnp.clip(queries, -40.0, 40.0)
    return (latent, queries)


def draw_latent_kv(key, part):
    return pair_draws(key)[0].astype(jnp.bfloat16)


def draw_queries(key, part):
    return pair_draws(key)[1].astype(jnp.bfloat16)


def place_ends(result, stream_key, smallest, high):
    spot = [jax.random.randint(jax.random.fold_in(stream_key, axis), (), 0, length) for axis, length in enumerate(result.shape)]
    main_axis = result.shape.index(max(result.shape))
    beside = spot[:main_axis] + [(spot[main_axis] + 1) % result.shape[main_axis]] + spot[main_axis + 1:]
    return result.at[tuple(spot)].set(smallest).at[tuple(beside)].set(high)


def spiked(entries, own_key, source, target, shards_of, factor):
    owner, partner = [(jnp.arange(entries.shape[dim]) // (entries.shape[dim] // shards_of)).reshape([-1 if axis == dim else 1 for axis in range(entries.ndim)]) for dim in (source, target)]
    chosen = jax.random.permutation(own_key, shards_of)[partner]
    strong = (owner == chosen) | (owner == (partner + shards_of // 2) % shards_of)
    return jnp.where(strong, factor * entries, entries)


def level_of(stream_key, dims, cuts, low, high):
    def one(dim, parts):
        steps = jax.random.uniform(jax.random.fold_in(jax.random.fold_in(stream_key, 6), dim), (parts,), jnp.float32, low / len(cuts), high / len(cuts))
        return jnp.repeat(jnp.exp(steps), dims[dim] // parts).reshape((-1,) + (1,) * (len(dims) - dim - 1))

    loudness = one(*cuts[0])
    for cut in cuts[1:]:
        loudness = loudness * one(*cut)
    return loudness


def scatter_about(own_key, dims, width, reach, shards=(), held_as=jnp.bfloat16):
    array = jax.random.normal(own_key, dims, jnp.float32) * width
    if len(shards) > 0:
        array = level_of(own_key, dims, shards, -0.22, 0.18) * array
    return jnp.clip(array, min=-reach, max=reach).astype(held_as)


def noise_with(rng, extent, spread, reach, pieces, heavy, kind=jnp.bfloat16):
    result = spread * jax.random.normal(rng, extent, jnp.float32)
    if pieces:
        result = result * level_of(rng, extent, pieces, -0.22, 0.18)
    return jnp.clip(spiked(result, jax.random.fold_in(rng, 3), *heavy), -reach, reach).astype(kind)


def setup_inputs(seed: int = 0, part: int = 0) -> dict:
    seeds = jax.random.split(jax.random.key(seed), 8)
    part_splits = jax.random.split(jax.random.fold_in(seeds[7], part), 8)
    queries = draw_queries(jax.random.fold_in(jax.random.fold_in(seeds[7], part), 71), part)
    latent_kv = draw_latent_kv(jax.random.fold_in(jax.random.fold_in(seeds[7], part), 71), part)
    adapter_ids = place_ends(jax.random.randint(part_splits[2], (TOKENS // ADP_BLOCK,), 0, ADAPTERS), jax.random.fold_in(part_splits[2], 1), 0, ADAPTERS - 1).astype(jnp.int32)
    value_up = scatter_about(seeds[3], (HEADS, LATENT, VHEAD), LATENT ** -0.5, 0.25, ((0, 4),))
    output_weight = noise_with(seeds[4], (HEADS * VHEAD, D), (HEADS * VHEAD) ** -0.5, 0.1875, ((0, 4),), (0, 1, 4, 2.0))
    adapter_down = scatter_about(seeds[5], (HEADS * VHEAD, ADAPTERS * RANK), (HEADS * VHEAD) ** -0.5, 0.125, ((0, 4),))
    adapter_up = scatter_about(seeds[6], (ADAPTERS * RANK, D), RANK ** -0.5, 1.5)
    return dict(queries=queries, latent_kv=latent_kv, adapter_ids=adapter_ids, value_up=value_up, output_weight=output_weight, adapter_down=adapter_down, adapter_up=adapter_up)


def mirror_position(rows, tok_dev, count):
    shard = rows // tok_dev
    within = rows % tok_dev
    half = tok_dev // 2
    return jnp.where(within < half, shard * half + within, (2 * count - 1 - shard) * half + within - half).astype(jnp.int32)

def reference(queries, latent_kv, adapter_ids, value_up, output_weight, adapter_down, adapter_up):
    score_scale = 1.0 / math.sqrt(NOPE + ROPE)
    position = mirror_position(jnp.arange(TOKENS, dtype=jnp.int32), TOK_DEV, N_SEQ)
    visible = position[None, :] <= position[:, None]
    latent = latent_kv[:, :LATENT]

    def one_head(index):
        query = lax.dynamic_index_in_dim(queries, index, 1, keepdims=False)
        scores = lax.dot_general(query, latent_kv, (((1,), (1,)), ((), ())), preferred_element_type=jnp.float32) * score_scale
        scores = jnp.where(visible, scores, -1e+30)
        row_max = lax.optimization_barrier(jnp.max(scores, axis=1, keepdims=True))
        weights = jnp.exp(scores - row_max)
        row_sum = lax.optimization_barrier(jnp.sum(weights, axis=1, keepdims=True))
        latent_out = jnp.dot(weights.astype(jnp.bfloat16), latent, preferred_element_type=jnp.float32) / row_sum
        return latent_out.astype(jnp.bfloat16)
    latent_out = lax.map(one_head, jnp.arange(HEADS, dtype=jnp.int32))
    value_out = jnp.einsum('hsl,hlv->shv', latent_out.astype(jnp.float32), value_up.astype(jnp.float32))
    value_out = value_out.astype(jnp.bfloat16).reshape(TOKENS, HEADS * VHEAD)
    projected = jnp.dot(value_out, output_weight, preferred_element_type=jnp.float32)
    rank_terms = jnp.dot(value_out, adapter_down, preferred_element_type=jnp.float32)
    token_ids = jnp.repeat(adapter_ids, ADP_BLOCK, total_repeat_length=TOKENS)
    owner = jnp.arange(ADAPTERS * RANK, dtype=jnp.int32) // RANK
    selector = (token_ids[:, None] == owner[None, :]).astype(jnp.float32)
    adapted = jnp.dot(rank_terms * selector, adapter_up.astype(jnp.float32), precision=lax.Precision.HIGHEST)
    return (projected + adapted).astype(jnp.bfloat16)
```

```python
import math

import jax
import jax.numpy as jnp
from jax import lax
from jax.sharding import PartitionSpec as P

ROPE = 64
NOPE = 128
ADAPTERS = 5
RANK = 16
ADP_BLOCK = 32


def block_start(shard, second, half, count):
    return jnp.where(second, (2 * count - 1 - shard) * half, shard * half)


def gather_latents(latent_kv):
    count = lax.axis_size("seq")
    heads = lax.axis_size("head")
    me = lax.axis_index("seq")
    core = lax.axis_index("head") % 2
    half = latent_kv.shape[0] // 2
    steps = jnp.arange(half, dtype=jnp.int32)
    own_half = lax.dynamic_slice_in_dim(latent_kv, core * half, half, 0)
    keys = [latent_kv]
    positions = [block_start(me, False, half, count) + steps, block_start(me, True, half, count) + steps]
    arrived = []
    for shift in range(1, count):
        pairs = []
        for source in range(count):
            target = (source - shift) % count
            for head in range(heads):
                if head % 2 == 0 or target < source:
                    pairs.append((source * heads + head, target * heads + head))
        arrived.append(lax.ppermute(own_half, ("seq", "head"), pairs))
        shard = (me + shift) % count
        positions.append(block_start(shard, core == 1, half, count) + steps)
    mine = jnp.concatenate(arrived, axis=0)
    other = lax.ppermute(mine, "head", [(head, head ^ 1) for head in range(heads)])
    for shift in range(1, count):
        shard = (me + shift) % count
        positions.append(block_start(shard, core == 0, half, count) + steps)
    return jnp.concatenate([latent_kv, mine, other], axis=0), jnp.concatenate(positions)


def body(queries, latent_kv, adapter_ids, value_up, output_weight, adapter_down, adapter_up):
    seq_count = lax.axis_size("seq")
    heads = lax.axis_size("head")
    own_index = lax.axis_index("seq")
    head_index = lax.axis_index("head")
    tok_rows, head_count, latent_width = queries.shape
    latent_dim = value_up.shape[1]
    half = tok_rows // 2
    score_scale = 1.0 / math.sqrt(NOPE + ROPE)
    query_rows = queries.transpose(1, 0, 2)
    steps = jnp.arange(half, dtype=jnp.int32)
    row_position = jnp.concatenate(
        [
            block_start(own_index, False, half, seq_count) + steps,
            block_start(own_index, True, half, seq_count) + steps,
        ]
    )
    carried, key_position = gather_latents(latent_kv)
    scores = (
        jnp.einsum("htl,ul->htu", query_rows, carried, preferred_element_type=jnp.float32)
        * score_scale
    )
    visible = key_position[None, :] <= row_position[:, None]
    scores = jnp.where(visible[None], scores, -1e30)
    row_max = jnp.max(scores, axis=2, keepdims=True)
    weights = jnp.exp(scores - row_max)
    row_sum = jnp.sum(weights, axis=2, keepdims=True)
    product = jnp.einsum(
        "htu,ul->htl",
        weights.astype(jnp.bfloat16),
        carried[:, :latent_dim],
        preferred_element_type=jnp.float32,
    )
    latent_out = (product / row_sum).astype(jnp.bfloat16)
    value_out = jnp.einsum("htl,hlv->thv", latent_out, value_up, preferred_element_type=jnp.float32)
    value_out = value_out.astype(jnp.bfloat16).reshape(tok_rows, head_count * value_up.shape[2])
    rank_part = jnp.dot(value_out, adapter_down, preferred_element_type=jnp.float32)
    owner = jnp.arange(ADAPTERS * RANK, dtype=jnp.int32) // RANK
    block_count = adapter_ids.shape[0]
    chosen = adapter_ids[:, None, None] == owner[None, None, :]
    chosen = jnp.broadcast_to(chosen, (block_count, ADP_BLOCK, ADAPTERS * RANK)).reshape(
        tok_rows, ADAPTERS * RANK
    )
    selected = jnp.where(chosen, rank_part, 0.0)
    high = selected.astype(jnp.bfloat16)
    low = (selected - high.astype(jnp.float32)).astype(jnp.bfloat16)
    left = jnp.concatenate([value_out, high, low], axis=1)
    right = jnp.concatenate([output_weight, adapter_up, adapter_up], axis=0)
    columns = adapter_up.shape[1] // heads
    pair, core = head_index // 2, head_index % 2
    pairs = heads // 2

    def share(owner_head):
        part = lax.dynamic_slice_in_dim(right, owner_head * columns, columns, 1)
        return jnp.dot(left, part, preferred_element_type=jnp.float32)

    order = [(pair + shift) % pairs for shift in range(pairs)]
    sent = jnp.concatenate([share(p * 2 + 1 - core).astype(jnp.bfloat16) for p in order], axis=1)
    received = lax.ppermute(sent, "head", [(head, head ^ 1) for head in range(heads)])
    kept = [
        share(p * 2 + core)
        + received[:, i * columns : (i + 1) * columns].astype(jnp.float32)
        for i, p in enumerate(order)
    ]
    mixed = kept[0]
    for shift in range(1, pairs):
        moves = [(head, (head + 2 * shift) % heads) for head in range(heads)]
        mixed += lax.ppermute(kept[shift].astype(jnp.bfloat16), "head", moves).astype(jnp.float32)
    return mixed.astype(jnp.bfloat16)


def solution(mesh):
    return jax.shard_map(
        body,
        mesh=mesh,
        in_specs=(
            P(("groups", "seq"), "head", None),
            P(("groups", "seq"), None),
            P(("groups", "seq")),
            P("head", None, None),
            P("head", None),
            P("head", None),
            P(),
        ),
        out_specs=P(("groups", "seq"), "head"),
        check_vma=False,
    )
```
